32 devices in a mesh: blk: 8 (over y, x, core), chan: 4 (over z).
Axes of the slice: x: 2, y: 2, z: 4, core: 2. Of those that a mesh axis runs over, the one named last changes fastest.
Arguments:
- pair_repr: bfloat16 [512, 512, 128], P('blk', 'chan'), may hold values from -6 to 6
- chain_lengths: int32 [8], replicated, may hold values from 48 to 64
- norm_gain: float32 [128], replicated, may hold values from 0.1 to 1.9
- norm_bias: float32 [128], replicated, may hold values from -3 to 3
- left_gate: bfloat16 [128, 128], replicated, may hold values from -0.5 to 0.5
- left_value: bfloat16 [128, 128], replicated, may hold values from -0.5 to 0.5
- right_gate: bfloat16 [128, 128], replicated, may hold values from -0.5 to 0.5
- right_value: bfloat16 [128, 128], replicated, may hold values from -0.5 to 0.5
- out_gain: float32 [128], replicated, may hold values from 0.1 to 1.9
- out_bias: float32 [128], replicated, may hold values from -3 to 3
- out_weight: bfloat16 [128, 128], replicated, may hold values from -0.5 to 0.5
- gate_weight: bfloat16 [128, 128], replicated, may hold values from -0.5 to 0.5
Outputs:
- pair_update: bfloat16 [512, 104, 128], P('blk', 'chan')
The draws below stay inside these ranges and needn't reach their ends.
Inputs may be any that keep to these rules, and one draw needn't show every extreme that they name: Chain slot s covers residues s * 64 to (s + 1) * 64 - 1, of which the first chain_lengths[s] are real and the rest padding.
All inputs are finite; a program needn't handle non-finite values.
Results may differ from the reference program's by a relative error of at most 0.0058.
Values may be sent and summed in bfloat16 or wider, within the bound.
A program may use at most 64 MiB of HBM per device.

```python
import jax
import jax.numpy as jnp
from jax import lax

C = 128
CH = 128
ROWS_DEV = 64
JD = 13
NCHAIN = 8
NRES = 512
SLOT = 64
J = 104
N_BLK = 8


def place_ends(result, rng, smallest, largest):
    longest = result.shape.index(max(result.shape))
    spots = []
    for shift in (0, 1):
        where = [jax.random.randint(jax.random.fold_in(rng, axis), (), 0, length) for axis, length in enumerate(result.shape)]
        where[longest] = (where[longest] + shift) % result.shape[longest]
        spots.append(tuple(where))
    return result.at[spots[0]].set(smallest).at[spots[1]].set(largest)


def levels(key, shape, pieces, smallest, high):
    gain, own = 1.0, jax.random.fold_in(key, 6)
    for dim, shards_of in pieces:
        draws = jnp.exp(jax.random.uniform(jax.random.fold_in(own, dim), (shards_of,), jnp.float32, smallest / len(pieces), high / len(pieces)))
        gain = gain * jnp.repeat(draws, shape[dim] // shards_of).reshape([-1 if axis == dim else 1 for axis in range(len(shape))])
    return gain


def bell_draw(own_key, extent, scale, limit, split=(), held_as=jnp.bfloat16):
    result = scale * jax.random.normal(own_key, extent, jnp.float32)
    if split:
        result = result * levels(own_key, extent, split, -0.22, 0.18)
    return jnp.clip(result, -limit, limit).astype(held_as)


def setup_inputs(seed: int = 0) -> dict:
    arg_keys = jax.random.split(jax.random.key(seed), 13)
    pair_repr = bell_draw(arg_keys[0], (NRES, NRES, C), 1.0, 6.0, ((0, 8), (1, 4)))
    chain_lengths = place_ends(jax.random.randint(arg_keys[1], (NCHAIN,), 3 * SLOT // 4, SLOT + 1), jax.random.fold_in(arg_keys[1], 1), 3 * SLOT // 4, SLOT).astype(jnp.int32)
    norm_gain = jnp.clip(1.0 + 0.18 * jax.random.normal(arg_keys[2], (C,), jnp.float32), 0.1, 1.9)
    norm_bias = bell_draw(arg_keys[3], (C,), 0.5, 3.0, (), jnp.float32)
    left_gate = bell_draw(arg_keys[4], (C, CH), C ** -0.5, 0.5)
    left_value = bell_draw(arg_keys[5], (C, CH), C ** -0.5, 0.5)
    right_gate = bell_draw(arg_keys[6], (C, CH), C ** -0.5, 0.5)
    right_value = bell_draw(arg_keys[7], (C, CH), C ** -0.5, 0.5)
    out_gain = jnp.clip(1.0 + 0.18 * jax.random.normal(arg_keys[8], (CH,), jnp.float32), 0.1, 1.9)
    out_bias = bell_draw(arg_keys[9], (CH,), 0.5, 3.0, (), jnp.float32)
    out_weight = bell_draw(arg_keys[10], (CH, C), CH ** -0.5, 0.5)
    gate_weight = bell_draw(arg_keys[11], (C, C), C ** -0.5, 0.5)
    return dict(pair_repr=pair_repr, chain_lengths=chain_lengths, norm_gain=norm_gain, norm_bias=norm_bias, left_gate=left_gate, left_value=left_value, right_gate=right_gate, right_value=right_value, out_gain=out_gain, out_bias=out_bias, out_weight=out_weight, gate_weight=gate_weight)


epsilon = 1e-05

def normalize(values, gain_vec, bias_vec):
    centre = lax.optimization_barrier(jnp.mean(values, axis=-1, keepdims=True))
    centred = values - centre
    spread_sq = lax.optimization_barrier(jnp.mean(centred * centred, axis=-1, keepdims=True))
    return centred * lax.rsqrt(spread_sq + epsilon) * gain_vec + bias_vec

def residue_mask(position, lengths, slot_size):
    chain_id = position // slot_size
    chain_table = jnp.arange(lengths.shape[0], dtype=jnp.int32)
    chain_len = lax.optimization_barrier(jnp.sum(jnp.where(chain_id[:, None] == chain_table[None, :], lengths[None, :], 0), axis=1))
    return (position % slot_size < chain_len).astype(jnp.float32)

def reference(pair_repr, chain_lengths, norm_gain, norm_bias, left_gate, left_value, right_gate, right_value, out_gain, out_bias, out_weight, gate_weight):
    position = jnp.arange(NRES, dtype=jnp.int32)
    residue = residue_mask(position, chain_lengths, SLOT)
    window = (jnp.arange(N_BLK, dtype=jnp.int32)[:, None] * ROWS_DEV + jnp.arange(JD, dtype=jnp.int32)[None, :]).reshape(-1)
    window_normed = normalize(pair_repr[window].astype(jnp.float32), norm_gain, norm_bias).astype(jnp.bfloat16)
    window_flat = window_normed.reshape(-1, C)
    right_mix = jax.nn.sigmoid(jnp.dot(window_flat, right_gate, preferred_element_type=jnp.float32)) * jnp.dot(window_flat, right_value, preferred_element_type=jnp.float32)
    right_mix = right_mix.reshape(J, NRES, CH) * residue[window][:, None, None] * residue[None, :, None]
    right_wide = jnp.transpose(right_mix.astype(jnp.bfloat16).astype(jnp.float32), (2, 0, 1))

    def row_block(block_id):
        start_row = block_id * ROWS_DEV
        block_pair = lax.dynamic_slice_in_dim(pair_repr, start_row, ROWS_DEV, 0)
        normed = normalize(block_pair.astype(jnp.float32), norm_gain, norm_bias).astype(jnp.bfloat16)
        flat_rows = normed.reshape(-1, C)
        left_mix = jax.nn.sigmoid(jnp.dot(flat_rows, left_gate, preferred_element_type=jnp.float32)) * jnp.dot(flat_rows, left_value, preferred_element_type=jnp.float32)
        row_real = lax.dynamic_slice_in_dim(residue, start_row, ROWS_DEV, 0)
        left_mix = left_mix.reshape(ROWS_DEV, NRES, CH) * row_real[:, None, None] * residue[None, :, None]
        left_wide = jnp.transpose(left_mix.astype(jnp.bfloat16).astype(jnp.float32), (2, 0, 1))
        product = jnp.einsum('cik,cjk->cij', left_wide, right_wide).astype(jnp.bfloat16).astype(jnp.float32)
        centre = lax.optimization_barrier(jnp.mean(product, axis=0, keepdims=True))
        centred = product - centre
        spread_sq = lax.optimization_barrier(jnp.mean(centred * centred, axis=0, keepdims=True))
        normed_product = (centred * lax.rsqrt(spread_sq + epsilon) * out_gain[:, None, None] + out_bias[:, None, None]).astype(jnp.bfloat16)
        update = jnp.einsum('cij,cd->ijd', normed_product.astype(jnp.float32), out_weight.astype(jnp.float32))
        gate_rows = normed[:, window]
        gate_value = jax.nn.sigmoid(jnp.einsum('ijd,de->ije', gate_rows.astype(jnp.float32), gate_weight.astype(jnp.float32)))
        return (gate_value * update).astype(jnp.bfloat16)
    blocks_out = lax.map(row_block, jnp.arange(N_BLK, dtype=jnp.int32))
    return blocks_out.reshape(NRES, J, C)
```

```python
import functools

import jax
import jax.numpy as jnp
from jax import lax
from jax.experimental import pallas as pl
from jax.experimental.pallas import tpu as pltpu
from jax.sharding import PartitionSpec as P

JD = 13
PAD = 16
EPS = 1e-05
F32 = jnp.float32
BF16 = jnp.bfloat16
NT = (((1,), (1,)), ((), ()))
TN = (((0,), (0,)), ((), ()))
NN = (((1,), (0,)), ((), ()))


def xor(a, b, n):
    total, bit = 0, 1
    while bit < n:
        total = total + bit * ((a // bit + b // bit) % 2)
        bit *= 2
    return total


def sigmoid(x):
    return 0.5 * jnp.tanh(0.5 * x) + 0.5


def layer_norm(x, gain, bias):
    centre = jnp.mean(x, axis=-1, keepdims=True)
    centred = x - centre
    spread = jnp.mean(centred * centred, axis=-1, keepdims=True)
    return centred * lax.rsqrt(spread + EPS) * gain + bias


def kernel(
    n_pos,
    slot_size,
    lens,
    pair_hbm,
    gain,
    bias,
    lgate,
    lvalue,
    rgate,
    rvalue,
    ogain,
    obias,
    oweight,
    gweight,
    out,
    pair,
    weights,
    right_all,
    left,
    r0,
    r1,
    work,
    send,
    recv,
    gate_in,
    gate_val,
    update,
    load_sem,
    rs_send,
    rs_recv,
    fw_send,
    fw_recv,
    ps_send,
    ps_recv,
):
    rows, cols, ch = pair.shape
    hid = lgate.shape[1]
    blk = lax.axis_index("blk")
    z = lax.axis_index("chan")
    q = blk // 2
    h = blk % 2
    partner = 2 * q + 1 - h

    load_a = pltpu.make_async_copy(
        pair_hbm.at[pl.ds(0, JD)], pair.at[pl.ds(0, JD)], load_sem.at[0]
    )
    load_b = pltpu.make_async_copy(
        pair_hbm.at[pl.ds(JD, rows - JD)], pair.at[pl.ds(JD, rows - JD)], load_sem.at[1]
    )
    load_a.start()
    load_b.start()

    barrier = pltpu.get_barrier_semaphore()
    for d in range(1, n_pos):
        pl.semaphore_signal(barrier, inc=1, device_id={"blk": 2 * xor(q, d, n_pos) + h})
        pl.semaphore_signal(barrier, inc=1, device_id={"chan": xor(z, d, n_pos)})
    pl.semaphore_signal(barrier, inc=1, device_id={"blk": partner})

    for n, w in enumerate((rgate, rvalue, lgate, lvalue)):
        weights[n * hid : (n + 1) * hid, :] = w[...].astype(F32).T.astype(BF16)

    col = z * cols + lax.broadcasted_iota(jnp.int32, (1, cols), 1)
    chain = col // slot_size
    chain_len = jnp.zeros_like(col)
    for s in range(lens.shape[0]):
        chain_len = jnp.where(chain == s, lens[s], chain_len)
    col_real = (col % slot_size < chain_len).astype(F32)

    def row_real(i):
        pos = blk * rows + i
        return jnp.where(pos % slot_size < lens[pos // slot_size], 1.0, 0.0).astype(F32)

    gain_v, bias_v = gain[...], bias[...]

    def norm_rows(i, count):
        x = pair[pl.ds(i, count)].astype(F32).reshape(count * cols, ch)
        return layer_norm(x, gain_v, bias_v).astype(BF16)

    load_a.wait()

    def right_row(m, carry):
        normed = norm_rows(m, 1)
        mix = lax.dot_general(weights[: 2 * hid, :], normed, NT, preferred_element_type=F32)
        val = sigmoid(mix[:hid]) * mix[hid:] * (col_real * row_real(m))
        right_all[blk, pl.ds(pl.multiple_of(m * hid, hid), hid), :] = val.astype(BF16)
        return carry

    lax.fori_loop(0, JD, right_row, 0)

    pl.semaphore_wait(barrier, 2 * (n_pos - 1) + 1)

    def right_copy(d):
        return pltpu.make_async_remote_copy(
            src_ref=right_all.at[blk],
            dst_ref=right_all.at[blk],
            send_sem=rs_send.at[d],
            recv_sem=rs_recv.at[d],
            device_id={"blk": 2 * xor(q, d, n_pos) + h},
        )

    def forward_copy(d):
        mine = 2 * xor(q, d, n_pos) + h
        return pltpu.make_async_remote_copy(
            src_ref=right_all.at[mine],
            dst_ref=right_all.at[mine],
            send_sem=fw_send.at[d],
            recv_sem=fw_recv.at[d],
            device_id={"blk": partner},
        )

    forward_copy(0).start()
    for d in range(1, n_pos):
        right_copy(d).start()

    load_b.wait()

    def left_rows(t, carry):
        i = 2 * t
        normed = norm_rows(i, 2)
        for u in range(2):
            for g in range(2):
                gate_in[g, i + u] = normed[u * cols + g * rows : u * cols + g * rows + PAD]
        mix = lax.dot_general(weights[2 * hid :, :], normed, NT, preferred_element_type=F32)
        val = sigmoid(mix[:hid]) * mix[hid:]
        for u in range(2):
            left[pl.ds(i + u, hid, stride=rows), :] = val[:, u * cols : (u + 1) * cols] * (
                col_real * row_real(i + u)
            )
        return carry

    lax.fori_loop(0, rows // 2, left_rows, 0)

    zero_rows = jnp.zeros((hid, cols), F32)
    for m in range(JD, PAD):
        r0[pl.ds(m, hid, stride=PAD), :] = zero_rows
        r1[pl.ds(m, hid, stride=PAD), :] = zero_rows

    def partial_copy(p):
        e = xor(z, p, n_pos)
        return pltpu.make_async_remote_copy(
            src_ref=send.at[p],
            dst_ref=recv.at[e],
            send_sem=ps_send.at[e],
            recv_sem=ps_recv.at[e],
            device_id={"chan": p},
        )

    def stage(d, carry):
        p = xor(q, d, n_pos)

        @pl.when(d > 0)
        def _():
            right_copy(d).wait_recv()
            forward_copy(d).start()

        forward_copy(d).wait_recv()
        for g, dst in enumerate((r0, r1)):
            for m in range(JD):
                dst[pl.ds(m, hid, stride=PAD), :] = right_all[
                    2 * p + g, m * hid : (m + 1) * hid, :
                ].astype(F32)

        def channels(t, inner):
            for u in range(8):
                c = 8 * t + u
                rr = pl.ds(pl.multiple_of(c * PAD, PAD), PAD)
                lhs = jnp.concatenate([r0[rr, :], r1[rr, :]], axis=1).astype(BF16)
                lc = left[pl.ds(pl.multiple_of(c * rows, rows), rows), :].astype(BF16)
                zc = jnp.zeros_like(lc)
                rhs = jnp.concatenate(
                    [jnp.concatenate([lc, zc], axis=1), jnp.concatenate([zc, lc], axis=1)], axis=0
                )
                work[pl.ds(c, PAD, stride=hid), :] = lax.dot_general(
                    lhs, rhs, NT, preferred_element_type=F32
                )
            return inner

        lax.fori_loop(0, hid // 8, channels, 0)
        for m in range(JD):
            send[p, m * hid : (m + 1) * hid, :] = work[m * hid : (m + 1) * hid, :].astype(BF16)

        @pl.when(p != z)
        def _():
            partial_copy(p).start()

        return carry

    lax.fori_loop(0, n_pos, stage, 0)

    def gates(g, carry):
        for t in range(2):
            x = gate_in[t, pl.ds(8 * g, 8)].reshape(8 * PAD, ch)
            mix = lax.dot_general(x, gweight[...], NN, preferred_element_type=F32)
            gate_val[t, pl.ds(8 * g, 8)] = sigmoid(mix).reshape(8, PAD, ch)
        return carry

    lax.fori_loop(0, rows // 8, gates, 0)

    ogain_v = jnp.broadcast_to(ogain[...], (2 * rows, hid)).T
    obias_v = jnp.broadcast_to(obias[...], (2 * rows, hid)).T
    zero_rows = jnp.zeros((2 * rows, ch), F32)
    for m in range(JD, PAD):
        update[pl.ds(m, 2 * rows, stride=PAD), :] = zero_rows

    for e in range(1, n_pos):
        partial_copy(xor(z, e, n_pos)).wait_recv()

    def finish(m, carry):
        here = pl.ds(pl.multiple_of(m * hid, hid), hid)
        total = send[z, here, :].astype(F32)
        for e in range(1, n_pos):
            total = total + recv[e, here, :].astype(F32)
        total = total.astype(BF16).astype(F32)
        centred = total - jnp.mean(total, axis=0, keepdims=True)
        spread = jnp.mean(centred * centred, axis=0, keepdims=True)
        normed = (centred * lax.rsqrt(spread + EPS) * ogain_v + obias_v).astype(BF16)
        update[pl.ds(m, 2 * rows, stride=PAD), :] = lax.dot_general(
            normed, oweight[...], TN, preferred_element_type=F32
        )
        return carry

    lax.fori_loop(0, JD, finish, 0)

    def write(g, carry):
        for t in range(2):
            at = pl.ds(pl.multiple_of((t * rows + 8 * g) * PAD, 8 * PAD), 8 * PAD)
            val = update[at, :].reshape(8, PAD, ch) * gate_val[t, pl.ds(8 * g, 8)]
            out[t, pl.ds(8 * g, 8)] = val.astype(BF16)
        return carry

    lax.fori_loop(0, rows // 8, write, 0)

    forward_copy(0).wait_send()
    for d in range(1, n_pos):
        right_copy(d).wait_send()
        forward_copy(d).wait_send()
        partial_copy(xor(z, d, n_pos)).wait_send()


def on_device(pair, lengths, gain, bias, lg, lv, rg, rv, ogain, obias, ow, gw):
    rows, cols, ch = pair.shape
    hid = lg.shape[1]
    n_blk = lax.axis_size("blk")
    n_pos = lax.axis_size("chan")
    assert n_blk == 2 * n_pos and cols == 2 * rows and n_pos & (n_pos - 1) == 0
    slot_size = rows * n_blk // lengths.shape[0]
    vmem = pl.BlockSpec(memory_space=pltpu.VMEM)
    dma = pltpu.SemaphoreType.DMA((n_pos,))
    block = (JD * hid, cols)
    out = pl.pallas_call(
        functools.partial(kernel, n_pos, slot_size),
        out_shape=jax.ShapeDtypeStruct((2, rows, PAD, ch), BF16),
        in_specs=[pl.BlockSpec(memory_space=pltpu.SMEM), pl.BlockSpec(memory_space=pl.ANY)]
        + [vmem] * 10,
        out_specs=vmem,
        scratch_shapes=[
            pltpu.VMEM((rows, cols, ch), BF16),
            pltpu.VMEM((4 * hid, ch), BF16),
            pltpu.VMEM((n_blk,) + block, BF16),
            pltpu.VMEM((hid * rows, cols), F32),
            pltpu.VMEM((hid * PAD, cols), F32),
            pltpu.VMEM((hid * PAD, cols), F32),
            pltpu.VMEM((PAD * hid, 2 * rows), F32),
            pltpu.VMEM((n_pos,) + block, BF16),
            pltpu.VMEM((n_pos,) + block, BF16),
            pltpu.VMEM((2, rows, PAD, ch), BF16),
            pltpu.VMEM((2, rows, PAD, ch), F32),
            pltpu.VMEM((2 * rows * PAD, ch), F32),
            pltpu.SemaphoreType.DMA((2,)),
            dma,
            dma,
            dma,
            dma,
            dma,
            dma,
        ],
        compiler_params=pltpu.CompilerParams(
            collective_id=0, has_side_effects=True, vmem_limit_bytes=60 * 2**20
        ),
    )(
        lengths,
        pair,
        gain.reshape(1, ch),
        bias.reshape(1, ch),
        lg,
        lv,
        rg,
        rv,
        ogain.reshape(1, hid),
        obias.reshape(1, hid),
        ow,
        gw,
    )
    return out[:, :, :JD].transpose(1, 0, 2, 3).reshape(rows, 2 * JD, ch)


def solution(mesh):
    in_specs = (P("blk", "chan", None),) + (P(),) * 11
    out_specs = P("blk", "chan", None)
    return jax.shard_map(
        on_device, mesh=mesh, in_specs=in_specs, out_specs=out_specs, check_vma=False
    )
```

```python
import functools

import jax
import jax.numpy as jnp
from jax import lax
from jax.experimental import pallas as pl
from jax.experimental.pallas import tpu as pltpu
from jax.sharding import PartitionSpec as P

JD = 13
PAD = 16
EPS = 1e-05
F32 = jnp.float32
BF16 = jnp.bfloat16
NT = (((1,), (1,)), ((), ()))
TN = (((0,), (0,)), ((), ()))
NN = (((1,), (0,)), ((), ()))


def xor(a, b, n):
    total, bit = 0, 1
    while bit < n:
        total = total + bit * ((a // bit + b // bit) % 2)
        bit *= 2
    return total


def reverse_bits(t, n):
    total, bit = 0, 1
    while bit < n:
        total = total + (n // 2 // bit) * ((t // bit) % 2)
        bit *= 2
    return total


def sigmoid(x):
    return 0.5 * jnp.tanh(0.5 * x) + 0.5


def layer_norm(x, gain, bias):
    centre = jnp.mean(x, axis=-1, keepdims=True)
    centred = x - centre
    spread = jnp.mean(centred * centred, axis=-1, keepdims=True)
    return centred * lax.rsqrt(spread + EPS) * gain + bias


def kernel(
    n_pos,
    slot_size,
    lens,
    pair_hbm,
    gain,
    bias,
    lgate,
    lvalue,
    rgate,
    rvalue,
    ogain,
    obias,
    oweight,
    gweight,
    out,
    pair,
    weights,
    right_all,
    left,
    r0,
    r1,
    work,
    send,
    own,
    recv,
    gate_in,
    gate_val,
    update,
    load_sem,
    rs_send,
    rs_recv,
    fw_send,
    fw_recv,
    ps_send,
    ps_recv,
):
    rows, cols, ch = pair.shape
    hid = lgate.shape[1]
    blk = lax.axis_index("blk")
    z = lax.axis_index("chan")
    q = blk // 2
    h = blk % 2
    partner = 2 * q + 1 - h

    load_a = pltpu.make_async_copy(
        pair_hbm.at[pl.ds(0, JD)], pair.at[pl.ds(0, JD)], load_sem.at[0]
    )
    load_b = pltpu.make_async_copy(
        pair_hbm.at[pl.ds(JD, rows - JD)], pair.at[pl.ds(JD, rows - JD)], load_sem.at[1]
    )
    load_a.start()
    load_b.start()

    barrier = pltpu.get_barrier_semaphore()
    for d in range(1, n_pos):
        pl.semaphore_signal(barrier, inc=1, device_id={"blk": 2 * xor(q, d, n_pos) + h})
        pl.semaphore_signal(barrier, inc=1, device_id={"chan": xor(z, d, n_pos)})
    pl.semaphore_signal(barrier, inc=1, device_id={"blk": partner})

    for n, w in enumerate((rgate, rvalue, lgate, lvalue)):
        weights[n * hid : (n + 1) * hid, :] = w[...].astype(F32).T.astype(BF16)

    col = z * cols + lax.broadcasted_iota(jnp.int32, (1, cols), 1)
    chain = col // slot_size
    chain_len = jnp.zeros_like(col)
    for s in range(lens.shape[0]):
        chain_len = jnp.where(chain == s, lens[s], chain_len)
    col_real = (col % slot_size < chain_len).astype(F32)

    def row_real(i):
        pos = blk * rows + i
        return jnp.where(pos % slot_size < lens[pos // slot_size], 1.0, 0.0).astype(F32)

    gain_v, bias_v = gain[...], bias[...]

    def norm_rows(i, count):
        x = pair[pl.ds(i, count)].astype(F32).reshape(count * cols, ch)
        return layer_norm(x, gain_v, bias_v).astype(BF16)

    load_a.wait()

    def right_row(m, carry):
        normed = norm_rows(m, 1)
        mix = lax.dot_general(weights[: 2 * hid, :], normed, NT, preferred_element_type=F32)
        val = sigmoid(mix[:hid]) * mix[hid:] * (col_real * row_real(m))
        right_all[blk, pl.ds(pl.multiple_of(m * hid, hid), hid), :] = val.astype(BF16)
        return carry

    lax.fori_loop(0, JD, right_row, 0)

    pl.semaphore_wait(barrier, 2 * (n_pos - 1) + 1)

    def right_copy(d):
        return pltpu.make_async_remote_copy(
            src_ref=right_all.at[blk],
            dst_ref=right_all.at[blk],
            send_sem=rs_send.at[d],
            recv_sem=rs_recv.at[d],
            device_id={"blk": 2 * xor(q, d, n_pos) + h},
        )

    def forward_copy(d):
        mine = 2 * xor(q, d, n_pos) + h
        return pltpu.make_async_remote_copy(
            src_ref=right_all.at[mine],
            dst_ref=right_all.at[mine],
            send_sem=fw_send.at[d],
            recv_sem=fw_recv.at[d],
            device_id={"blk": partner},
        )

    forward_copy(0).start()
    for t in range(1, n_pos):
        right_copy(reverse_bits(t, n_pos)).start()

    load_b.wait()

    def left_rows(t, carry):
        i = 8 * t
        normed = norm_rows(i, 8)
        for u in range(8):
            for g in range(2):
                at = pl.ds(pl.multiple_of((i + u) * 2 * PAD, 2 * PAD) + g * JD, JD)
                gate_in[at, :] = normed[
                    u * cols + g * rows : u * cols + g * rows + JD
                ].astype(F32)
        mix = lax.dot_general(weights[2 * hid :, :], normed, NT, preferred_element_type=F32)
        val = sigmoid(mix[:hid]) * mix[hid:]
        for u in range(8):
            left[pl.ds(i + u, hid, stride=rows + 8), :] = val[:, u * cols : (u + 1) * cols] * (
                col_real * row_real(i + u)
            )
        return carry

    lax.fori_loop(0, rows // 8, left_rows, 0)

    def partial_copy(p):
        e = xor(z, p, n_pos)
        return pltpu.make_async_remote_copy(
            src_ref=send.at[p],
            dst_ref=recv.at[e],
            send_sem=ps_send.at[e],
            recv_sem=ps_recv.at[e],
            device_id={"chan": p},
        )

    def stage(t, carry):
        d = reverse_bits(t, n_pos)
        p = xor(q, d, n_pos)

        @pl.when(d > 0)
        def _():
            right_copy(d).wait_recv()
            forward_copy(d).start()

        forward_copy(d).wait_recv()
        for g, dst in enumerate((r0, r1)):
            for m in range(JD):
                dst[pl.ds(m, hid, stride=PAD), :] = right_all[
                    2 * p + g, m * hid : (m + 1) * hid, :
                ].astype(F32)

        def channels(t, inner):
            for u in range(32):
                c = 32 * t + u
                rr = pl.ds(pl.multiple_of(c * PAD, PAD), PAD)
                lhs = jnp.concatenate([r0[rr, :], r1[rr, :]], axis=0).astype(BF16)
                lc = left[pl.ds(pl.multiple_of(c * (rows + 8), 8), rows), :].astype(BF16)
                o = lax.dot_general(lhs, lc, NT, preferred_element_type=F32)
                work[pl.ds(c, PAD, stride=hid + 8), :] = jnp.concatenate([o[:PAD], o[PAD:]], axis=1)
            return inner

        lax.fori_loop(0, hid // 32, channels, 0)
        @pl.when(p == z)
        def _():
            for m in range(JD):
                own[m * hid : (m + 1) * hid, :] = work[m * (hid + 8) : m * (hid + 8) + hid, :]

        @pl.when(p != z)
        def _():
            for m in range(JD):
                send[p, m * hid : (m + 1) * hid, :] = work[
                    m * (hid + 8) : m * (hid + 8) + hid, :
                ].astype(BF16)
            partial_copy(p).start()

        return carry

    lax.fori_loop(0, n_pos, stage, 0)

    wide = 8 * 2 * PAD

    def gates(g, carry):
        at = pl.ds(pl.multiple_of(g * wide, wide), wide)
        mix = lax.dot_general(
            gate_in[at, :].astype(BF16), gweight[...], NN, preferred_element_type=F32
        )
        gate_val[at, :] = sigmoid(mix)
        return carry

    lax.fori_loop(0, rows // 8, gates, 0)

    ogain_v = jnp.broadcast_to(ogain[...], (2 * rows, hid)).T
    obias_v = jnp.broadcast_to(obias[...], (2 * rows, hid)).T
    for e in range(1, n_pos):
        partial_copy(xor(z, e, n_pos)).wait_recv()

    def finish(m):
        here = slice(m * hid, (m + 1) * hid)
        total = own[here, :]
        for e in range(1, n_pos):
            total = total + recv[e, here, :].astype(F32)
        total = total.astype(BF16).astype(F32)
        centred = total - jnp.mean(total, axis=0, keepdims=True)
        spread = jnp.mean(centred * centred, axis=0, keepdims=True)
        normed = (centred * lax.rsqrt(spread + EPS) * ogain_v + obias_v).astype(BF16)
        val = lax.dot_general(normed, oweight[...], TN, preferred_element_type=F32)
        for g in range(2):
            update[pl.ds(g * JD + m, rows, stride=2 * PAD), :] = val[g * rows : (g + 1) * rows]

    for m in range(JD):
        finish(m)

    def write(g, carry):
        at = pl.ds(pl.multiple_of(g * wide, wide), wide)
        val = (update[at, :] * gate_val[at, :]).reshape(8, 2 * PAD, ch)
        out[pl.ds(pl.multiple_of(8 * g, 8), 8)] = val[:, : 2 * JD].astype(BF16)
        return carry

    lax.fori_loop(0, rows // 8, write, 0)

    forward_copy(0).wait_send()
    for d in range(1, n_pos):
        right_copy(d).wait_send()
        forward_copy(d).wait_send()
        partial_copy(xor(z, d, n_pos)).wait_send()


def on_device(pair, lengths, gain, bias, lg, lv, rg, rv, ogain, obias, ow, gw):
    rows, cols, ch = pair.shape
    hid = lg.shape[1]
    n_blk = lax.axis_size("blk")
    n_pos = lax.axis_size("chan")
    assert n_blk == 2 * n_pos and cols == 2 * rows and n_pos & (n_pos - 1) == 0
    slot_size = rows * n_blk // lengths.shape[0]
    vmem = pl.BlockSpec(memory_space=pltpu.VMEM)
    dma = pltpu.SemaphoreType.DMA((n_pos,))
    block = (JD * hid, cols)
    return pl.pallas_call(
        functools.partial(kernel, n_pos, slot_size),
        out_shape=jax.ShapeDtypeStruct((rows, 2 * JD, ch), BF16),
        in_specs=[pl.BlockSpec(memory_space=pltpu.SMEM), pl.BlockSpec(memory_space=pl.ANY)]
        + [vmem] * 10,
        out_specs=vmem,
        scratch_shapes=[
            pltpu.VMEM((rows, cols, ch), BF16),
            pltpu.VMEM((4 * hid, ch), BF16),
            pltpu.VMEM((n_blk,) + block, BF16),
            pltpu.VMEM((hid * (rows + 8), cols), F32),
            pltpu.VMEM((hid * PAD, cols), F32),
            pltpu.VMEM((hid * PAD, cols), F32),
            pltpu.VMEM((PAD * (hid + 8), 2 * rows), F32),
            pltpu.VMEM((n_pos,) + block, BF16),
            pltpu.VMEM(block, F32),
            pltpu.VMEM((n_pos,) + block, BF16),
            pltpu.VMEM((2 * rows * PAD, ch), F32),
            pltpu.VMEM((2 * rows * PAD, ch), F32),
            pltpu.VMEM((2 * rows * PAD, ch), F32),
            pltpu.SemaphoreType.DMA((2,)),
            dma,
            dma,
            dma,
            dma,
            dma,
            dma,
        ],
        compiler_params=pltpu.CompilerParams(
            collective_id=0, has_side_effects=True, vmem_limit_bytes=60 * 2**20
        ),
    )(
        lengths,
        pair,
        gain.reshape(1, ch),
        bias.reshape(1, ch),
        lg,
        lv,
        rg,
        rv,
        ogain.reshape(1, hid),
        obias.reshape(1, hid),
        ow,
        gw,
    )


def solution(mesh):
    in_specs = (P("blk", "chan", None),) + (P(),) * 11
    out_specs = P("blk", "chan", None)
    return jax.shard_map(
        on_device, mesh=mesh, in_specs=in_specs, out_specs=out_specs, check_vma=False
    )
```

```python
import functools

import jax
import jax.numpy as jnp
from jax import lax
from jax.experimental import pallas as pl
from jax.experimental.pallas import tpu as pltpu
from jax.sharding import PartitionSpec as P

JD = 13
PAD = 16
EPS = 1e-05
F32 = jnp.float32
BF16 = jnp.bfloat16
NT = (((1,), (1,)), ((), ()))
TN = (((0,), (0,)), ((), ()))
NN = (((1,), (0,)), ((), ()))


def xor(a, b, n):
    total, bit = 0, 1
    while bit < n:
        total = total + bit * ((a // bit + b // bit) % 2)
        bit *= 2
    return total


def reverse_bits(t, n):
    total, bit = 0, 1
    while bit < n:
        total = total + (n // 2 // bit) * ((t // bit) % 2)
        bit *= 2
    return total


def sigmoid(x):
    return 0.5 * jnp.tanh(0.5 * x) + 0.5


def layer_norm(x, gain, bias):
    centre = jnp.mean(x, axis=-1, keepdims=True)
    centred = x - centre
    spread = jnp.mean(centred * centred, axis=-1, keepdims=True)
    return centred * lax.rsqrt(spread + EPS) * gain + bias


def kernel(
    n_pos,
    slot_size,
    lens,
    pair_hbm,
    gain,
    bias,
    lgate,
    lvalue,
    rgate,
    rvalue,
    ogain,
    obias,
    oweight,
    gweight,
    out,
    pair,
    weights,
    right_all,
    left,
    r0,
    r1,
    work,
    send,
    own,
    recv,
    gate_in,
    gate_val,
    update,
    load_sem,
    rs_send,
    rs_recv,
    fw_send,
    fw_recv,
    ps_send,
    ps_recv,
    relay,
    rl_send,
    rl_recv,
):
    rows, cols, ch = pair.shape
    hid = lgate.shape[1]
    blk = lax.axis_index("blk")
    z = lax.axis_index("chan")
    q = blk // 2
    h = blk % 2
    partner = 2 * q + 1 - h

    load_a = pltpu.make_async_copy(
        pair_hbm.at[pl.ds(0, JD)], pair.at[pl.ds(0, JD)], load_sem.at[0]
    )
    load_b = pltpu.make_async_copy(
        pair_hbm.at[pl.ds(JD, rows - JD)], pair.at[pl.ds(JD, rows - JD)], load_sem.at[1]
    )
    load_a.start()
    load_b.start()

    barrier = pltpu.get_barrier_semaphore()
    for d in range(1, n_pos):
        pl.semaphore_signal(barrier, inc=1, device_id={"blk": 2 * xor(q, d, n_pos) + h})
        pl.semaphore_signal(barrier, inc=1, device_id={"chan": xor(z, d, n_pos)})
    pl.semaphore_signal(barrier, inc=1, device_id={"blk": partner})

    for n, w in enumerate((rgate, rvalue, lgate, lvalue)):
        weights[n * hid : (n + 1) * hid, :] = w[...].astype(F32).T.astype(BF16)

    col = z * cols + lax.broadcasted_iota(jnp.int32, (1, cols), 1)
    chain = col // slot_size
    chain_len = jnp.zeros_like(col)
    for s in range(lens.shape[0]):
        chain_len = jnp.where(chain == s, lens[s], chain_len)
    col_real = (col % slot_size < chain_len).astype(F32)

    def row_real(i):
        pos = blk * rows + i
        return jnp.where(pos % slot_size < lens[pos // slot_size], 1.0, 0.0).astype(F32)

    gain_v, bias_v = gain[...], bias[...]

    def norm_rows(i, count):
        x = pair[pl.ds(i, count)].astype(F32).reshape(count * cols, ch)
        return layer_norm(x, gain_v, bias_v).astype(BF16)

    load_a.wait()

    def right_row(m, carry):
        normed = norm_rows(m, 1)
        mix = lax.dot_general(weights[: 2 * hid, :], normed, NT, preferred_element_type=F32)
        val = sigmoid(mix[:hid]) * mix[hid:] * (col_real * row_real(m))
        right_all[blk, pl.ds(pl.multiple_of(m * hid, hid), hid), :] = val.astype(BF16)
        return carry

    for m in range(JD):
        right_row(m, 0)

    pl.semaphore_wait(barrier, 2 * (n_pos - 1) + 1)

    def right_copy(d):
        return pltpu.make_async_remote_copy(
            src_ref=right_all.at[blk],
            dst_ref=right_all.at[blk],
            send_sem=rs_send.at[d],
            recv_sem=rs_recv.at[d],
            device_id={"blk": 2 * xor(q, d, n_pos) + h},
        )

    def forward_copy(d):
        mine = 2 * xor(q, d, n_pos) + h
        return pltpu.make_async_remote_copy(
            src_ref=right_all.at[mine],
            dst_ref=right_all.at[mine],
            send_sem=fw_send.at[d],
            recv_sem=fw_recv.at[d],
            device_id={"blk": partner},
        )

    forward_copy(0).start()
    for t in range(1, n_pos):
        right_copy(reverse_bits(t, n_pos)).start()

    load_b.wait()

    def left_rows(t, carry):
        i = 8 * t
        normed = norm_rows(i, 8)
        for u in range(8):
            for g in range(2):
                at = pl.ds(pl.multiple_of((i + u) * 2 * PAD, 2 * PAD) + g * JD, JD)
                gate_in[at, :] = normed[
                    u * cols + g * rows : u * cols + g * rows + JD
                ].astype(F32)
        mix = lax.dot_general(weights[2 * hid :, :], normed, NT, preferred_element_type=F32)
        val = sigmoid(mix[:hid]) * mix[hid:]
        for u in range(8):
            left[pl.ds(i + u, hid, stride=rows + 8), :] = val[:, u * cols : (u + 1) * cols] * (
                col_real * row_real(i + u)
            )
        return carry

    lax.fori_loop(0, rows // 8, left_rows, 0)

    def partial_copy(p):
        e = xor(z, p, n_pos)
        return pltpu.make_async_remote_copy(
            src_ref=send.at[p],
            dst_ref=recv.at[e],
            send_sem=ps_send.at[e],
            recv_sem=ps_recv.at[e],
            device_id={"chan": p},
        )

    wide = 8 * 2 * PAD

    def gates(g, carry):
        at = pl.ds(pl.multiple_of(g * wide, wide), wide)
        mix = lax.dot_general(
            gate_in[at, :].astype(BF16), gweight[...], NN, preferred_element_type=F32
        )
        gate_val[at, :] = sigmoid(mix)
        return carry

    last = n_pos - 1
    half = n_pos // 2

    def relayed(source, p):
        ends = ((source == 0) & (p >= half)) | ((source == last) & (p < half))
        return ends & ((p + q) % 2 == 1)

    next_in = jnp.where(z == 0, 1, jnp.where(z == last, last - 1, -1))
    behind = jnp.where(z == 1, 0, jnp.where(z == last - 1, last, -1))

    def relay_copy(p):
        return pltpu.make_async_remote_copy(
            src_ref=send.at[p],
            dst_ref=relay.at[p],
            send_sem=rl_send.at[p],
            recv_sem=rl_recv.at[p],
            device_id={"chan": jnp.where(z < half, 1, last - 1)},
        )

    def stage(t, carry):
        d = reverse_bits(t, n_pos)
        p = xor(q, d, n_pos)

        @pl.when(d > 0)
        def _():
            right_copy(d).wait_recv()
            forward_copy(d).start()

        forward_copy(d).wait_recv()
        for g, dst in enumerate((r0, r1)):
            for m in range(JD):
                dst[pl.ds(m, hid, stride=PAD + 8), :] = right_all[
                    2 * p + g, m * hid : (m + 1) * hid, :
                ].astype(F32)

        def channels(t, inner):
            for u in range(32):
                c = 32 * t + u
                rr = pl.ds(pl.multiple_of(c * (PAD + 8), 8), PAD)
                lhs = jnp.concatenate([r0[rr, :], r1[rr, :]], axis=0).astype(BF16)
                lc = left[pl.ds(pl.multiple_of(c * (rows + 8), 8), rows), :].astype(BF16)
                o = lax.dot_general(lhs, lc, NT, preferred_element_type=F32)
                work[pl.ds(c, PAD, stride=hid + 8), :] = jnp.concatenate([o[:PAD], o[PAD:]], axis=1)
            return inner

        lax.fori_loop(0, hid // 32, channels, 0)
        @pl.when(p == z)
        def _():
            for m in range(JD):
                own[m * hid : (m + 1) * hid, :] = work[m * (hid + 8) : m * (hid + 8) + hid, :]

        @pl.when(p != z)
        def _():
            for m in range(JD):
                send[p, m * hid : (m + 1) * hid, :] = work[
                    m * (hid + 8) : m * (hid + 8) + hid, :
                ].astype(BF16)

            @pl.when(relayed(z, p))
            def _():
                relay_copy(p).start()

            later = (p == next_in) | relayed(behind, p)

            @pl.when(jnp.logical_not(relayed(z, p) | later))
            def _():
                partial_copy(p).start()

        return carry

    lax.fori_loop(0, n_pos, stage, 0)

    @pl.when(next_in >= 0)
    def _():
        partial_copy(next_in).start()

    def pass_on(t, carry):
        p = xor(q, reverse_bits(half + t, n_pos), n_pos)

        @pl.when(relayed(behind, p))
        def _():
            relay_copy(p).wait_recv()
            for m in range(JD):
                here = slice(m * hid, (m + 1) * hid)
                send[p, here, :] = (
                    send[p, here, :].astype(F32) + relay[p, here, :].astype(F32)
                ).astype(BF16)
            partial_copy(p).start()

        return carry

    lax.fori_loop(0, rows // 8, gates, 0)
    lax.fori_loop(0, half, pass_on, 0)

    ogain_v = jnp.broadcast_to(ogain[...], (2 * rows, hid)).T
    obias_v = jnp.broadcast_to(obias[...], (2 * rows, hid)).T
    for e in range(1, n_pos):
        source = xor(z, e, n_pos)

        @pl.when(jnp.logical_not(relayed(source, z)))
        def _():
            partial_copy(source).wait_recv()

    def finish(m):
        here = slice(m * hid, (m + 1) * hid)
        total = own[here, :]
        for e in range(1, n_pos):
            more = recv[e, here, :].astype(F32)
            total = total + jnp.where(relayed(xor(z, e, n_pos), z), 0.0, more)
        total = total.astype(BF16).astype(F32)
        centred = total - jnp.mean(total, axis=0, keepdims=True)
        spread = jnp.mean(centred * centred, axis=0, keepdims=True)
        normed = (centred * lax.rsqrt(spread + EPS) * ogain_v + obias_v).astype(BF16)
        val = lax.dot_general(normed, oweight[...], TN, preferred_element_type=F32)
        for g in range(2):
            update[pl.ds(g * JD + m, rows, stride=2 * PAD), :] = val[g * rows : (g + 1) * rows]

    for m in range(JD):
        finish(m)

    def write(g, carry):
        at = pl.ds(pl.multiple_of(g * wide, wide), wide)
        val = (update[at, :] * gate_val[at, :]).reshape(8, 2 * PAD, ch)
        out[pl.ds(pl.multiple_of(8 * g, 8), 8)] = val[:, : 2 * JD].astype(BF16)
        return carry

    lax.fori_loop(0, rows // 8, write, 0)

    forward_copy(0).wait_send()
    for d in range(1, n_pos):
        right_copy(d).wait_send()
        forward_copy(d).wait_send()
        target = xor(z, d, n_pos)

        @pl.when(relayed(z, target))
        def _():
            relay_copy(target).wait_send()

        @pl.when(jnp.logical_not(relayed(z, target)))
        def _():
            partial_copy(target).wait_send()


def on_device(pair, lengths, gain, bias, lg, lv, rg, rv, ogain, obias, ow, gw):
    rows, cols, ch = pair.shape
    hid = lg.shape[1]
    n_blk = lax.axis_size("blk")
    n_pos = lax.axis_size("chan")
    assert n_blk == 2 * n_pos and cols == 2 * rows and n_pos >= 4 and n_pos & (n_pos - 1) == 0
    slot_size = rows * n_blk // lengths.shape[0]
    vmem = pl.BlockSpec(memory_space=pltpu.VMEM)
    dma = pltpu.SemaphoreType.DMA((n_pos,))
    block = (JD * hid, cols)
    return pl.pallas_call(
        functools.partial(kernel, n_pos, slot_size),
        out_shape=jax.ShapeDtypeStruct((rows, 2 * JD, ch), BF16),
        in_specs=[pl.BlockSpec(memory_space=pltpu.SMEM), pl.BlockSpec(memory_space=pl.ANY)]
        + [vmem] * 10,
        out_specs=vmem,
        scratch_shapes=[
            pltpu.VMEM((rows, cols, ch), BF16),
            pltpu.VMEM((4 * hid, ch), BF16),
            pltpu.VMEM((n_blk,) + block, BF16),
            pltpu.VMEM((hid * (rows + 8), cols), F32),
            pltpu.VMEM((hid * (PAD + 8), cols), F32),
            pltpu.VMEM((hid * (PAD + 8), cols), F32),
            pltpu.VMEM((PAD * (hid + 8), 2 * rows), F32),
            pltpu.VMEM((n_pos,) + block, BF16),
            pltpu.VMEM(block, F32),
            pltpu.VMEM((n_pos,) + block, BF16),
            pltpu.VMEM((2 * rows * PAD, ch), F32),
            pltpu.VMEM((2 * rows * PAD, ch), F32),
            pltpu.VMEM((2 * rows * PAD, ch), F32),
            pltpu.SemaphoreType.DMA((2,)),
            dma,
            dma,
            dma,
            dma,
            dma,
            dma,
            pltpu.VMEM((n_pos,) + block, BF16),
            dma,
            dma,
        ],
        compiler_params=pltpu.CompilerParams(
            collective_id=0, has_side_effects=True, vmem_limit_bytes=60 * 2**20
        ),
    )(
        lengths,
        pair,
        gain.reshape(1, ch),
        bias.reshape(1, ch),
        lg,
        lv,
        rg,
        rv,
        ogain.reshape(1, hid),
        obias.reshape(1, hid),
        ow,
        gw,
    )


def solution(mesh):
    in_specs = (P("blk", "chan", None),) + (P(),) * 11
    out_specs = P("blk", "chan", None)
    return jax.shard_map(
        on_device, mesh=mesh, in_specs=in_specs, out_specs=out_specs, check_vma=False
    )
```
